32 devices in a mesh: row: 4 (over x, core), col: 8 (over z, y).
Axes of the slice: x: 2, y: 2, z: 4, core: 2. Of those that a mesh axis runs over, the one named last changes fastest.
Arguments:
- tensor: float32 [1024, 128, 1024], P('row', 'col'), may hold values from -6 to 6
- start_basis: float32 [1024, 256], P(('row', 'col')), may hold values from -6 to 6
Outputs:
- scaled_basis: float32 [1024, 256], P(('row', 'col'))
- core: float32 [1024, 128, 256], P('row', 'col')
The draws below stay inside these ranges and needn't reach their ends.
All inputs are finite; a program needn't handle non-finite values.
Results may differ from the reference program's by a relative error of at most 0.0003.
Values sent between devices are 32-bit elements; how exact they have to be, the bound alone decides.
A program may use at most 128 MiB of HBM per device.

```python
import math
import jax
import jax.numpy as jnp
from jax import lax

N2 = 1024
K = 256
PASSES = 2
N1 = 1024
N3 = 128


def raised(drawn, own_key, source, target, shards_of, factor):
    def block_of(axis_at):
        return (jnp.arange(drawn.shape[axis_at]) // (drawn.shape[axis_at] // shards_of)).reshape((-1,) + (1,) * (drawn.ndim - 1 - axis_at))

    first = jax.random.permutation(own_key, shards_of)[block_of(target)]
    far = (block_of(target) + shards_of // 2) % shards_of
    return jnp.where((block_of(source) == first) | (block_of(source) == far), factor * drawn, drawn)


def block_levels(stream_key, dims, split, smallest, high):
    level, own = 1.0, jax.random.fold_in(stream_key, 6)
    for axis_at, shards_of in split:
        draws = jnp.exp(jax.random.uniform(jax.random.fold_in(own, axis_at), (shards_of,), jnp.float32, smallest / len(split), high / len(split)))
        level = level * jnp.repeat(draws, dims[axis_at] // shards_of).reshape([-1 if axis == axis_at else 1 for axis in range(len(dims))])
    return level


def bell_draw(stream_key, extent, scale, reach, cuts=(), kind=jnp.bfloat16):
    level = block_levels(stream_key, extent, cuts, -0.22, 0.18) if cuts else 1.0
    result = jax.random.normal(stream_key, extent, jnp.float32) * scale * level
    return jnp.minimum(jnp.maximum(result, -reach), reach).astype(kind)


def noise_with(own_key, extent, scale, reach, shards, heavy, kind=jnp.bfloat16):
    result = scale * jax.random.normal(own_key, extent, jnp.float32)
    if shards:
        result = result * block_levels(own_key, extent, shards, -0.22, 0.18)
    return jnp.clip(raised(result, jax.random.fold_in(own_key, 3), *heavy), -reach, reach).astype(kind)


def setup_inputs(seed: int = 0) -> dict:
    key_of = jax.random.split(jax.random.key(seed), 3)
    tensor = noise_with(key_of[0], (N1, N3, N2), 1.0, 6.0, ((0, 4), (1, 8)), (1, 2, 8, 2.0), jnp.float32)
    start_basis = bell_draw(key_of[1], (N2, K), 1.0, 6.0, ((0, 32),), jnp.float32)
    return {"tensor": tensor, "start_basis": start_basis}


def orthonormal(tall_block):
    gram_part = jnp.dot(tall_block.T.astype(jnp.float32), tall_block.astype(jnp.float32), precision=lax.Precision.HIGHEST, preferred_element_type=jnp.float32)
    cholesky_low = jnp.linalg.cholesky(gram_part)
    return jax.scipy.linalg.solve_triangular(cholesky_low, tall_block.T, lower=True).T

def reference(tensor, start_basis):
    subspace = start_basis
    for repeat in range(PASSES):
        coefficients = jnp.einsum('ikj,jr->ikr', tensor, subspace, precision=lax.Precision.HIGHEST)
        product = jnp.einsum('ikj,ikr->jr', tensor, coefficients, precision=lax.Precision.HIGHEST)
        subspace = orthonormal(product)
    core = jnp.einsum('ikj,jr->ikr', tensor, subspace, precision=lax.Precision.HIGHEST)
    return (math.sqrt(N2) * subspace, core)
```

```python
import functools
import math

import jax
import jax.numpy as jnp
from jax import lax
from jax.experimental import pallas as pl
from jax.experimental.pallas import tpu as pltpu
from jax.sharding import PartitionSpec as P

PASSES = 2
TILE = 256
PANEL = 32
HIGHEST = lax.Precision.HIGHEST


def split(x):
    high = x.astype(jnp.bfloat16)
    return high, (x - high.astype(jnp.float32)).astype(jnp.bfloat16)


def dot0(a, b):
    return lax.dot_general(a, b, (((0,), (0,)), ((), ())), preferred_element_type=jnp.float32)


def exact(a, b, dims):
    return lax.dot_general(a, b, (dims, ((), ())), precision=HIGHEST, preferred_element_type=jnp.float32)


def gram_kernel(x_ref, out_ref):
    @pl.when(pl.program_id(0) == 0)
    def _():
        out_ref[...] = jnp.zeros_like(out_ref)

    high, low = split(x_ref[...])
    order = x_ref.shape[1]
    at = 0
    for start in range(0, order, TILE):
        own_high, own_low = high[:, start : start + TILE], low[:, start : start + TILE]
        rest_high, rest_low = high[:, start:], low[:, start:]
        part = dot0(own_high, rest_high) + dot0(own_high, rest_low) + dot0(own_low, rest_high)
        out_ref[:, at : at + order - start] += part
        at += order - start


def packed_gram(slab):
    rows, order = slab.shape
    width = sum(order - start for start in range(0, order, TILE))
    chunk = 512
    return pl.pallas_call(
        gram_kernel,
        grid=(rows // chunk,),
        in_specs=[pl.BlockSpec((chunk, order), lambda i: (i, 0))],
        out_specs=pl.BlockSpec((TILE, width), lambda i: (0, 0)),
        out_shape=jax.ShapeDtypeStruct((TILE, width), jnp.float32),
        compiler_params=pltpu.CompilerParams(dimension_semantics=("arbitrary",)),
        name="packed_gram",
    )(slab)


def factor(gram_ref, done_ref):
    count = gram_ref.shape[0]
    sub = lax.broadcasted_iota(jnp.int32, (8, 128), 0)
    lanes = count // 128
    for c0 in range(0, count, PANEL):
        rows = lax.broadcasted_iota(jnp.int32, (PANEL, count), 0)
        cols = lax.broadcasted_iota(jnp.int32, (PANEL, count), 1)
        unit = jnp.where(cols == rows + c0, 1.0, 0.0).astype(jnp.float32)
        panel = jnp.concatenate([gram_ref[c0 : c0 + PANEL, :], unit], axis=1)
        if c0:
            panel = panel - exact(done_ref[:c0, c0 : c0 + PANEL], done_ref[:c0, :], ((0,), (0,)))
        groups = PANEL // 8
        x = [
            [panel[8 * g : 8 * g + 8, 128 * v : 128 * v + 128] for v in range(2 * lanes)]
            for g in range(groups)
        ]
        for t in range(groups):
            col = {}
            for g in range(t, groups):
                for k in range(8):
                    at = c0 + 8 * t + k
                    col[g, k] = jnp.broadcast_to(x[g][at // 128][:, at % 128 : at % 128 + 1], (8, 128))
            pivots = jnp.ones((8, 128), jnp.float32)
            for k in range(8):
                pivot = jnp.broadcast_to(col[t, k][k : k + 1, :], (8, 128))
                pivots = jnp.where(sub == k, pivot, pivots)
                if k == 7 and t == groups - 1:
                    continue
                inverse = 1.0 / pivot
                heads = {j: jnp.broadcast_to(col[t, j][k : k + 1, :], (8, 128)) for j in range(k + 1, 8)}
                tops = [jnp.broadcast_to(x[t][v][k : k + 1, :], (8, 128)) for v in range(2 * lanes)]
                for g in range(t, groups):
                    scale = col[g, k] * inverse
                    if g == t:
                        scale = jnp.where(sub > k, scale, 0.0)
                    for j in range(k + 1, 8):
                        col[g, j] = col[g, j] - scale * heads[j]
                    for v in range(2 * lanes):
                        x[g][v] = x[g][v] - scale * tops[v]
            root = 1.0 / jnp.sqrt(pivots)
            for v in range(2 * lanes):
                done_ref[c0 + 8 * t : c0 + 8 * t + 8, 128 * v : 128 * v + 128] = x[t][v] * root


def subspace_kernel(packed_ref, start_ref, out_ref, whole, tall, gram, done):
    order = start_ref.shape[0]
    at = 0
    for start in range(0, order, TILE):
        for other in range(start, order, TILE):
            block = packed_ref[:, at : at + TILE]
            whole[start : start + TILE, other : other + TILE] = block
            if other > start:
                whole[other : other + TILE, start : start + TILE] = block.T
            at += TILE
    out_ref[...] = start_ref[...]

    def step(_, carry):
        tall[...] = exact(whole[...], out_ref[...], ((1,), (0,)))
        gram[...] = exact(tall[...], tall[...], ((0,), (0,)))
        factor(gram, done)
        out_ref[...] = exact(tall[...], done[:, gram.shape[0] :], ((1,), (1,)))
        return carry

    lax.fori_loop(0, PASSES, step, 0)


def iterate(packed, start):
    order, count = start.shape
    return pl.pallas_call(
        subspace_kernel,
        in_specs=[pl.BlockSpec(memory_space=pltpu.VMEM)] * 2,
        out_specs=pl.BlockSpec(memory_space=pltpu.VMEM),
        out_shape=jax.ShapeDtypeStruct((order, count), jnp.float32),
        scratch_shapes=[
            pltpu.VMEM((order, order), jnp.float32),
            pltpu.VMEM((order, count), jnp.float32),
            pltpu.VMEM((count, count), jnp.float32),
            pltpu.VMEM((count, 2 * count), jnp.float32),
        ],
        name="iterate",
    )(packed, start)


def core_kernel(x_ref, basis_ref, out_ref):
    high, low = split(x_ref[...])
    basis_high, basis_low = split(basis_ref[...])
    dot = functools.partial(jnp.dot, preferred_element_type=jnp.float32)
    out_ref[...] = dot(high, basis_high) + dot(high, basis_low) + dot(low, basis_high)


def core_of(slab, basis):
    rows, order = slab.shape
    count = basis.shape[1]
    chunk = 512
    return pl.pallas_call(
        core_kernel,
        grid=(rows // chunk,),
        in_specs=[
            pl.BlockSpec((chunk, order), lambda i: (i, 0)),
            pl.BlockSpec((order, count), lambda i: (0, 0)),
        ],
        out_specs=pl.BlockSpec((chunk, count), lambda i: (i, 0)),
        out_shape=jax.ShapeDtypeStruct((rows, count), jnp.float32),
        compiler_params=pltpu.CompilerParams(dimension_semantics=("arbitrary",)),
        name="core",
    )(slab, basis)


def body(tensor, start_basis):
    own_count = start_basis.shape[0]
    device_slot = lax.axis_index("row") * lax.axis_size("col") + lax.axis_index("col")
    start = lax.all_gather(start_basis, ("row", "col"), axis=0, tiled=True)
    slab = tensor.reshape(-1, tensor.shape[-1])
    packed = lax.psum(packed_gram(slab), ("row", "col"))
    subspace = iterate(packed, start)
    own_slice = lax.dynamic_slice_in_dim(subspace, device_slot * own_count, own_count, 0)
    scaled_rows = math.sqrt(subspace.shape[0]) * own_slice
    core_block = core_of(slab, subspace)
    return (scaled_rows, core_block.reshape(*tensor.shape[:2], -1))


def solution(mesh):
    return jax.shard_map(
        body,
        mesh=mesh,
        in_specs=(P("row", "col", None), P(("row", "col"), None)),
        out_specs=(P(("row", "col"), None), P("row", "col", None)),
        check_vma=False,
    )
```

```python
import functools
import math

import jax
import jax.numpy as jnp
from jax import lax
from jax.experimental import pallas as pl
from jax.experimental.pallas import tpu as pltpu
from jax.sharding import PartitionSpec as P

PASSES = 2
TILE = 256
PANEL = 32
HIGHEST = lax.Precision.HIGHEST


def split(x):
    high = x.astype(jnp.bfloat16)
    return high, (x - high.astype(jnp.float32)).astype(jnp.bfloat16)


def dot0(a, b):
    return lax.dot_general(a, b, (((0,), (0,)), ((), ())), preferred_element_type=jnp.float32)


def exact(a, b, dims):
    return lax.dot_general(a, b, (dims, ((), ())), precision=HIGHEST, preferred_element_type=jnp.float32)


def gram_kernel(x_ref, out_ref):
    @pl.when(pl.program_id(0) == 0)
    def _():
        out_ref[...] = jnp.zeros_like(out_ref)

    high, low = split(x_ref[...])
    order = x_ref.shape[1]
    at = 0
    for start in range(0, order, TILE):
        own_high, own_low = high[:, start : start + TILE], low[:, start : start + TILE]
        rest_high, rest_low = high[:, start:], low[:, start:]
        part = dot0(own_high, rest_high) + dot0(own_high, rest_low) + dot0(own_low, rest_high)
        out_ref[:, at : at + order - start] += part
        at += order - start


def packed_gram(slab):
    rows, order = slab.shape
    width = sum(order - start for start in range(0, order, TILE))
    chunk = 512
    return pl.pallas_call(
        gram_kernel,
        grid=(rows // chunk,),
        in_specs=[pl.BlockSpec((chunk, order), lambda i: (i, 0))],
        out_specs=pl.BlockSpec((TILE, width), lambda i: (0, 0)),
        out_shape=jax.ShapeDtypeStruct((TILE, width), jnp.float32),
        compiler_params=pltpu.CompilerParams(dimension_semantics=("arbitrary",)),
        name="packed_gram",
    )(slab)


def factor(gram_ref, done_ref):
    count = gram_ref.shape[0]
    sub = lax.broadcasted_iota(jnp.int32, (8, 128), 0)
    lanes = count // 128
    for c0 in range(0, count, PANEL):
        rows = lax.broadcasted_iota(jnp.int32, (PANEL, count), 0)
        cols = lax.broadcasted_iota(jnp.int32, (PANEL, count), 1)
        unit = jnp.where(cols == rows + c0, 1.0, 0.0).astype(jnp.float32)
        panel = jnp.concatenate([gram_ref[c0 : c0 + PANEL, :], unit], axis=1)
        if c0:
            panel = panel - exact(done_ref[:c0, c0 : c0 + PANEL], done_ref[:c0, :], ((0,), (0,)))
        groups = PANEL // 8
        x = [
            [panel[8 * g : 8 * g + 8, 128 * v : 128 * v + 128] for v in range(2 * lanes)]
            for g in range(groups)
        ]
        for t in range(groups):
            col = {}
            for g in range(t, groups):
                for k in range(8):
                    at = c0 + 8 * t + k
                    col[g, k] = jnp.broadcast_to(x[g][at // 128][:, at % 128 : at % 128 + 1], (8, 128))
            pivots = jnp.ones((8, 128), jnp.float32)
            for k in range(8):
                pivot = jnp.broadcast_to(col[t, k][k : k + 1, :], (8, 128))
                pivots = jnp.where(sub == k, pivot, pivots)
                if k == 7 and t == groups - 1:
                    continue
                inverse = 1.0 / pivot
                heads = {j: jnp.broadcast_to(col[t, j][k : k + 1, :], (8, 128)) for j in range(k + 1, 8)}
                tops = [jnp.broadcast_to(x[t][v][k : k + 1, :], (8, 128)) for v in range(2 * lanes)]
                for g in range(t, groups):
                    scale = col[g, k] * inverse
                    if g == t:
                        scale = jnp.where(sub > k, scale, 0.0)
                    for j in range(k + 1, 8):
                        col[g, j] = col[g, j] - scale * heads[j]
                    for v in range(2 * lanes):
                        x[g][v] = x[g][v] - scale * tops[v]
            root = 1.0 / jnp.sqrt(pivots)
            for v in range(2 * lanes):
                done_ref[c0 + 8 * t : c0 + 8 * t + 8, 128 * v : 128 * v + 128] = x[t][v] * root


def subspace_kernel(packed_ref, start_ref, out_ref, whole, tall, gram, done):
    order = start_ref.shape[0]
    at = 0
    for start in range(0, order, TILE):
        for other in range(start, order, TILE):
            block = packed_ref[:, at : at + TILE]
            whole[start : start + TILE, other : other + TILE] = block
            if other > start:
                whole[other : other + TILE, start : start + TILE] = block.T
            at += TILE
    out_ref[...] = start_ref[...]

    def step(_, carry):
        tall[...] = exact(whole[...], out_ref[...], ((1,), (0,)))
        gram[...] = exact(tall[...], tall[...], ((0,), (0,)))
        factor(gram, done)
        out_ref[...] = exact(tall[...], done[:, gram.shape[0] :], ((1,), (1,)))
        return carry

    lax.fori_loop(0, PASSES, step, 0)


def iterate(packed, start):
    order, count = start.shape
    return pl.pallas_call(
        subspace_kernel,
        in_specs=[pl.BlockSpec(memory_space=pltpu.VMEM)] * 2,
        out_specs=pl.BlockSpec(memory_space=pltpu.VMEM),
        out_shape=jax.ShapeDtypeStruct((order, count), jnp.float32),
        scratch_shapes=[
            pltpu.VMEM((order, order), jnp.float32),
            pltpu.VMEM((order, count), jnp.float32),
            pltpu.VMEM((count, count), jnp.float32),
            pltpu.VMEM((count, 2 * count), jnp.float32),
        ],
        name="iterate",
    )(packed, start)


def core_kernel(x_ref, basis_ref, out_ref):
    high, low = split(x_ref[...])
    basis_high, basis_low = split(basis_ref[...])
    dot = functools.partial(jnp.dot, preferred_element_type=jnp.float32)
    out_ref[...] = dot(high, basis_high) + dot(high, basis_low) + dot(low, basis_high)


def core_of(slab, basis):
    rows, order = slab.shape
    count = basis.shape[1]
    chunk = 512
    return pl.pallas_call(
        core_kernel,
        grid=(rows // chunk,),
        in_specs=[
            pl.BlockSpec((chunk, order), lambda i: (i, 0)),
            pl.BlockSpec((order, count), lambda i: (0, 0)),
        ],
        out_specs=pl.BlockSpec((chunk, count), lambda i: (i, 0)),
        out_shape=jax.ShapeDtypeStruct((rows, count), jnp.float32),
        compiler_params=pltpu.CompilerParams(dimension_semantics=("arbitrary",)),
        name="core",
    )(slab, basis)


def body(tensor, start_basis):
    own_count = start_basis.shape[0]
    device_slot = lax.axis_index("row") * lax.axis_size("col") + lax.axis_index("col")
    half = start_basis.shape[1] // 2
    left = lax.all_gather(start_basis[:, :half], ("row", "col"), axis=0, tiled=True)
    right_own, left = lax.optimization_barrier((start_basis[:, half:], left))
    right = lax.all_gather(right_own, ("row", "col"), axis=0, tiled=True)
    start = jnp.concatenate([left, right], axis=1)
    slab = tensor.reshape(-1, tensor.shape[-1])
    packed = lax.psum(packed_gram(slab), ("row", "col"))
    subspace = iterate(packed, start)
    own_slice = lax.dynamic_slice_in_dim(subspace, device_slot * own_count, own_count, 0)
    scaled_rows = math.sqrt(subspace.shape[0]) * own_slice
    core_block = core_of(slab, subspace)
    return (scaled_rows, core_block.reshape(*tensor.shape[:2], -1))


def solution(mesh):
    return jax.shard_map(
        body,
        mesh=mesh,
        in_specs=(P("row", "col", None), P(("row", "col"), None)),
        out_specs=(P(("row", "col"), None), P("row", "col", None)),
        check_vma=False,
    )
```
